32 devices in a mesh: tok: 32 (over z, y, x, core), head: 1.
Axes of the slice: x: 2, y: 2, z: 4, core: 2. Of those that a mesh axis runs over, the one named last changes fastest.
Arguments:
- queries: bfloat16 [32768, 4096], P('tok', 'head'), may hold values from -6 to 6
- keys: bfloat16 [32768, 4096], P('tok', 'head'), may hold values from -6 to 6
- values: bfloat16 [32768, 4096], P('tok', 'head'), may hold values from -6 to 6
- rates: float32 [8, 32768], P('head', 'tok'), may hold values from 0.02 to 0.2
- w_gate: bfloat16 [8, 512, 512], P('head', 'tok'), may hold values from -0.25 to 0.25
- w_up: bfloat16 [8, 512, 512], P('head', 'tok'), may hold values from -0.25 to 0.25
- w_down: bfloat16 [8, 512, 512], P('head', 'tok'), may hold values from -0.25 to 0.25
- out_gain: float32 [4096], P('head'), may hold values from 0.1 to 1.9
Outputs:
- mixed: bfloat16 [32768, 4096], P('tok', 'head')
The draws below stay inside these ranges and needn't reach their ends.
All inputs are finite; a program needn't handle non-finite values.
Results may differ from the reference program's by a relative error of at most 0.009.
Values may be sent and summed in bfloat16 or wider, within the bound.
No kernel may reach another device: no remote copies, remote signals or barrier semaphores. Data moves between devices by JAX's collectives and lax.ppermute only.
A program may use at most 192 MiB of HBM per device.

```python
import math
import jax
import jax.numpy as jnp
from jax import lax

HEADS = 8
DH = 512
D = 4096
TOKENS = 32768


def steps_of(stream_key, dims, cuts, low, largest):
    factor_of = 1.0
    for axis_at, shards_of in cuts:
        draws = jax.random.uniform(jax.random.fold_in(jax.random.fold_in(stream_key, 6), axis_at), (shards_of,), jnp.float32, low / len(cuts), largest / len(cuts))
        factor_of = factor_of * jnp.repeat(jnp.exp(draws), dims[axis_at] // shards_of).reshape((-1,) + (1,) * (len(dims) - 1 - axis_at))
    return factor_of


def gaussian(stream_key, dims, width, reach, cuts=(), kind=jnp.bfloat16):
    factor_of = steps_of(stream_key, dims, cuts, -0.22, 0.18) if cuts else 1.0
    drawn = jax.random.normal(stream_key, dims, jnp.float32) * width * factor_of
    return jnp.minimum(jnp.maximum(drawn, -reach), reach).astype(kind)


def setup_inputs(seed: int = 0) -> dict:
    key_of = jax.random.split(jax.random.key(seed), 9)
    return {
        "queries": gaussian(key_of[0], (TOKENS, D), 1.0, 6.0, ((0, 32),)),
        "keys": gaussian(key_of[1], (TOKENS, D), 1.0, 6.0, ((0, 32),)),
        "values": gaussian(key_of[2], (TOKENS, D), 1.0, 6.0, ((0, 32),)),
        "rates": jnp.clip(jnp.exp(math.log(0.2) - 2.3025851 * jax.random.uniform(key_of[3], (HEADS, TOKENS), jnp.float32) ** steps_of(key_of[3], (HEADS, TOKENS), ((1, 32),), -0.2, 0.2)), 0.02, 0.2),
        "w_gate": gaussian(key_of[4], (HEADS, DH, DH), DH ** -0.5, 0.25, ((1, 32),)),
        "w_up": gaussian(key_of[5], (HEADS, DH, DH), DH ** -0.5, 0.25, ((1, 32),)),
        "w_down": gaussian(key_of[6], (HEADS, DH, DH), DH ** -0.5, 0.25, ((1, 32),)),
        "out_gain": jnp.clip(1.0 + 0.18 * jax.random.normal(key_of[7], (D,), jnp.float32), 0.1, 1.9),
    }


def normalize(weights):
    return (weights * lax.rsqrt(lax.optimization_barrier(jnp.sum(weights * weights, axis=0, keepdims=True)) + 1e-06)).astype(jnp.bfloat16)

def activate(gate):
    sigma = jax.nn.sigmoid(gate)
    return (gate * sigma, sigma * (1.0 + gate * (1.0 - sigma)))

def reference(queries, keys, values, rates, w_gate, w_up, w_down, out_gain):
    pieces = []
    for head in range(HEADS):
        low = head * DH
        key_rows = keys[:, low:low + DH]
        value_rows = values[:, low:low + DH].astype(jnp.float32)
        query_rows = queries[:, low:low + DH]
        scale = rates[head].astype(jnp.float32)[:, None] / math.sqrt(TOKENS)
        first, third, second = (w_gate[head], w_up[head], w_down[head])
        gate = jnp.dot(key_rows, first, preferred_element_type=jnp.float32)
        up = jnp.dot(key_rows, third, preferred_element_type=jnp.float32)
        act, slope = activate(gate)
        hidden = (act * up).astype(jnp.bfloat16)
        fitted = jnp.dot(hidden, second, preferred_element_type=jnp.float32)
        error = (scale * (fitted - value_rows)).astype(jnp.bfloat16)
        grad_down = jnp.dot(hidden.T, error, preferred_element_type=jnp.float32)
        back = jnp.dot(error, second.T, preferred_element_type=jnp.float32)
        grad_gate = jnp.dot(key_rows.T, (back * up * slope).astype(jnp.bfloat16), preferred_element_type=jnp.float32)
        grad_up = jnp.dot(key_rows.T, (back * act).astype(jnp.bfloat16), preferred_element_type=jnp.float32)
        new_first = normalize(first.astype(jnp.float32) - grad_gate)
        new_third = normalize(third.astype(jnp.float32) - grad_up)
        new_second = normalize(second.astype(jnp.float32) - grad_down)
        query_gate = jnp.dot(query_rows, new_first, preferred_element_type=jnp.float32)
        query_up = jnp.dot(query_rows, new_third, preferred_element_type=jnp.float32)
        query_act, unused = activate(query_gate)
        query_hidden = (query_act * query_up).astype(jnp.bfloat16)
        pieces.append(jnp.dot(query_hidden, new_second, preferred_element_type=jnp.float32))
    applied = jnp.concatenate(pieces, axis=1)
    square = lax.optimization_barrier(jnp.sum(applied * applied, axis=1, keepdims=True)) / D
    return (applied * lax.rsqrt(square + 1e-06) * out_gain.astype(jnp.float32)[None, :]).astype(jnp.bfloat16)
```

```python
import functools
import math

import jax
import jax.numpy as jnp
from jax import lax
from jax.experimental import pallas as pl
from jax.experimental.pallas import tpu as pltpu
from jax.sharding import PartitionSpec as P

F32 = jnp.float32
BF16 = jnp.bfloat16


def activate(gate):
    sigma = jax.nn.sigmoid(gate)
    return (gate * sigma, sigma * (1.0 + gate * (1.0 - sigma)))


def apply_heads(inputs, weights):
    return jnp.einsum("thi,hij->thj", inputs, weights, preferred_element_type=F32)


def scaled_columns(updated, norms):
    return (updated * lax.rsqrt(norms + 1e-06)[:, None, :]).astype(BF16)


def query_pass(query_rows, new_gate, new_up, new_down):
    query_gate = apply_heads(query_rows, new_gate)
    query_up = apply_heads(query_rows, new_up)
    query_act, unused = activate(query_gate)
    query_hidden = (query_act * query_up).astype(BF16)
    return apply_heads(query_hidden, new_down)


def plain_shards(queries, keys, values, rates, w_gate, w_up, w_down, out_gain):
    heads = w_gate.shape[0]
    width = w_gate.shape[2]
    rows = keys.shape[0]
    total = rows * lax.axis_size("tok")
    full_gate, full_up, full_down = (
        lax.all_gather(w_gate, "tok", axis=1, tiled=True),
        lax.all_gather(w_up, "tok", axis=1, tiled=True),
        lax.all_gather(w_down, "tok", axis=1, tiled=True),
    )
    key_rows = keys.reshape(rows, heads, width)
    value_rows = values.reshape(rows, heads, width).astype(F32)
    query_rows = queries.reshape(rows, heads, width)
    scale = rates.T / math.sqrt(total)
    gate = apply_heads(key_rows, full_gate)
    up = apply_heads(key_rows, full_up)
    act, slope = activate(gate)
    hidden = (act * up).astype(BF16)
    fitted = apply_heads(hidden, full_down)
    error = (scale[:, :, None] * (fitted - value_rows)).astype(BF16)
    grad_down = jnp.einsum("thi,thj->hij", hidden, error, preferred_element_type=F32)
    back = jnp.einsum("thj,hij->thi", error, full_down, preferred_element_type=F32)
    grad_gate = jnp.einsum(
        "thi,thj->hij", key_rows, (back * up * slope).astype(BF16), preferred_element_type=F32
    )
    grad_up = jnp.einsum("thi,thj->hij", key_rows, (back * act).astype(BF16), preferred_element_type=F32)
    sum_gate, sum_up, sum_down = lax.psum((grad_gate, grad_up, grad_down), "tok")
    updated = [
        full_gate.astype(F32) - sum_gate,
        full_up.astype(F32) - sum_up,
        full_down.astype(F32) - sum_down,
    ]
    new_gate, new_up, new_down = [scaled_columns(item, jnp.sum(item * item, axis=1)) for item in updated]
    applied = query_pass(query_rows, new_gate, new_up, new_down)
    flat = applied.reshape(rows, heads * width)
    square = lax.psum(jnp.sum(flat * flat, axis=1), "head")
    inverse = lax.rsqrt(square / (heads * width * lax.axis_size("head")) + 1e-06)
    return (flat * inverse[:, None] * out_gain[None, :]).astype(BF16)


def masks_of(chips, odd):
    planes = max(chips // 4, 1)
    masks = []
    for bit in reversed(range(planes.bit_length() - 1)):
        masks.append(((2 << bit) - 1) * 4)
    return masks + ([1, 2] if odd else [2, 1])


def mask_of(piece, masks):
    value = 0
    for bit, mask in enumerate(masks):
        if piece >> bit & 1:
            value ^= mask
    return value


def flip(array, mask, devices):
    return lax.ppermute(array, "tok", [(i, i ^ mask) for i in range(devices)])


def gather_pieces(piece, masks, devices):
    own = piece[None]
    for mask in masks[:-1]:
        own = jnp.concatenate([own, flip(own, 2 * mask, devices)], axis=0)
    return own, flip(own, 2 * masks[-1], devices)


def add(a, b):
    return a.astype(F32) + b.astype(F32)


def reduce_pieces(keep, send, masks, devices):
    got = flip(send, 2 * masks[-1], devices)
    for mask in reversed(masks[:-1]):
        half = keep.shape[0] // 2
        send = add(keep[half:], got[half:]).astype(BF16)
        keep = add(keep[:half], got[:half]).astype(BF16)
        got = flip(send, 2 * mask, devices)
    return add(keep[0], got[0])


def assemble(place_ref, own_ref, got_ref, wide_ref, down_ref, masks):
    pieces, _, rows, width = own_ref.shape
    chip = place_ref[1]
    for piece in range(2 * pieces):
        source = own_ref if piece < pieces else got_ref
        at = pl.multiple_of((chip ^ mask_of(piece, masks)) * rows, rows)
        index = piece % pieces
        wide_ref[pl.ds(at, rows), :width] = source[index, 0]
        wide_ref[pl.ds(at, rows), width:] = source[index, 1]
        down_ref[pl.ds(at, rows), :] = source[index, 2]


def contract_rows(a, b):
    return lax.dot_general(a, b, (((0,), (0,)), ((), ())), preferred_element_type=F32)


def learn_kernel(
    place_ref, k_own, k_got, v_own, v_got, scale_ref, own_ref, got_ref,
    keep_ref, send_ref, wide, down, grad_wide, grad_down, *, head, masks, tiles,
):
    step = pl.program_id(0)
    width = down.shape[1]

    @pl.when(step == 0)
    def _():
        assemble(place_ref, own_ref, got_ref, wide, down, masks)
        grad_wide[...] = jnp.zeros_like(grad_wide)
        grad_down[...] = jnp.zeros_like(grad_down)

    def tile(k_ref, v_ref):
        k = k_ref[...]
        both = jnp.dot(k, wide[...], preferred_element_type=F32)
        gate = both[:, :width]
        up = both[:, width:]
        sigma = 1.0 / (1.0 + jnp.exp(-gate))
        act = gate * sigma
        hidden = (act * up).astype(BF16)
        fitted = jnp.dot(hidden, down[...], preferred_element_type=F32)
        scale = scale_ref[:, head : head + 1]
        error = (scale * (fitted - v_ref[...].astype(F32))).astype(BF16)
        grad_down[...] += contract_rows(hidden, error)
        back = lax.dot_general(
            error, down[...], (((1,), (1,)), ((), ())), preferred_element_type=F32
        )
        slope = sigma + act * (1.0 - sigma)
        dgate = (back * up * slope).astype(BF16)
        dup = (back * act).astype(BF16)
        grad_wide[:, :width] += contract_rows(k, dgate)
        grad_wide[:, width:] += contract_rows(k, dup)

    @pl.when(step < tiles)
    def _():
        tile(k_own, v_own)

    @pl.when(step >= tiles)
    def _():
        tile(k_got, v_got)

    @pl.when(step == 2 * tiles - 1)
    def _():
        pieces, _, rows, _ = keep_ref.shape
        chip = place_ref[1]
        for piece in range(2 * pieces):
            target = keep_ref if piece < pieces else send_ref
            at = pl.multiple_of((chip ^ mask_of(piece, masks)) * rows, rows)
            index = piece % pieces
            target[index, 0] = grad_wide[pl.ds(at, rows), :width].astype(BF16)
            target[index, 1] = grad_wide[pl.ds(at, rows), width:].astype(BF16)
            target[index, 2] = grad_down[pl.ds(at, rows), :].astype(BF16)


def answer_kernel(
    place_ref, q_own, q_got, own_ref, got_ref, out_own, out_other,
    wide, down, wide_norm, down_norm, *, masks, tiles,
):
    step = pl.program_id(0)
    width = down.shape[1]

    @pl.when(step == 0)
    def _():
        assemble(place_ref, own_ref, got_ref, wide, down, masks)
        first = wide[...].astype(F32)
        wide_norm[...] = lax.rsqrt(jnp.sum(first * first, axis=0, keepdims=True) + 1e-06)
        second = down[...].astype(F32)
        down_norm[...] = lax.rsqrt(jnp.sum(second * second, axis=0, keepdims=True) + 1e-06)

    def tile(q_ref, out_ref):
        both = jnp.dot(q_ref[...], wide[...], preferred_element_type=F32) * wide_norm[...]
        gate = both[:, :width]
        act = gate / (1.0 + jnp.exp(-gate))
        hidden = (act * both[:, width:]).astype(BF16)
        out = jnp.dot(hidden, down[...], preferred_element_type=F32) * down_norm[...]
        out_ref[...] = out.astype(BF16)

    @pl.when(step < tiles)
    def _():
        tile(q_got, out_other)

    @pl.when(step >= tiles)
    def _():
        tile(q_own, out_own)


def norm_kernel(place_ref, *refs, heads):
    own, got, gain_ref, out_ref = refs[:heads], refs[heads : 2 * heads], refs[-2], refs[-1]
    width = own[0].shape[1]
    total = 0.0
    for ref in own + got:
        block = ref[...].astype(F32)
        total = total + jnp.sum(block * block, axis=1, keepdims=True)
    inverse = lax.rsqrt(total / (2 * heads * width) + 1e-06)

    def write(first, second):
        for index, ref in enumerate(first + second):
            at = slice(index * width, (index + 1) * width)
            out_ref[:, at] = (ref[...].astype(F32) * inverse * gain_ref[:, at]).astype(BF16)

    @pl.when(place_ref[0] == 0)
    def _():
        write(own, got)

    @pl.when(place_ref[0] != 0)
    def _():
        write(got, own)


def tile_of(rows, most):
    size = most
    while rows % size:
        size //= 2
    return size


def fast_shards(queries, keys, values, rates, w_gate, w_up, w_down, out_gain):
    heads, share, width = w_gate.shape
    rows = keys.shape[0]
    devices = lax.axis_size("tok")
    chips = devices // 2
    mine = heads // 2
    total = rows * devices
    place = lax.axis_index("tok")
    core = place % 2
    chip = place // 2
    where = jnp.stack([core, chip]).astype(jnp.int32)

    def halves(array, axis):
        size = array.shape[axis] // 2
        keep = lax.dynamic_slice_in_dim(array, core * size, size, axis)
        give = lax.dynamic_slice_in_dim(array, (1 - core) * size, size, axis)
        return keep, flip(give, 1, devices)

    stacked = jnp.stack([w_gate, w_up, w_down], axis=1)
    kept, got = halves(stacked, 0)
    pair = jnp.where(core == 0, jnp.stack([kept, got], 2), jnp.stack([got, kept], 2))
    chip_rows = pair.reshape(mine, 3, 2 * share, width)

    masks = [masks_of(chips, head % 2) for head in range(mine)]
    weights = [gather_pieces(chip_rows[head], masks[head], devices) for head in range(mine)]

    own_rates, got_rates = halves(rates, 0)
    scale = jnp.concatenate([own_rates, got_rates], axis=1).T / math.sqrt(total)
    key_got = halves(keys, 1)[1]
    value_got = halves(values, 1)[1]
    query_got = halves(queries, 1)[1]

    size = tile_of(rows, 512)
    tiles = rows // size
    piece_rows = 2 * share
    half = chips // 2

    def pieces_spec():
        return pl.BlockSpec((half, 3, piece_rows, width), lambda t, s: (0, 0, 0, 0))

    def own_spec(head, late):
        if late:
            return pl.BlockSpec((size, width), lambda t, s: (jnp.maximum(t - tiles, 0), s[0] * mine + head))
        return pl.BlockSpec((size, width), lambda t, s: (jnp.minimum(t, tiles - 1), s[0] * mine + head))

    def got_spec(head, late):
        if late:
            return pl.BlockSpec((size, width), lambda t, s: (jnp.maximum(t - tiles, 0), head))
        return pl.BlockSpec((size, width), lambda t, s: (jnp.minimum(t, tiles - 1), head))

    def learn(head):
        own, got = weights[head]
        pieces = jax.ShapeDtypeStruct((half, 3, piece_rows, width), BF16)
        return pl.pallas_call(
            functools.partial(learn_kernel, head=head, masks=masks[head], tiles=tiles),
            out_shape=(pieces, pieces),
            grid_spec=pltpu.PrefetchScalarGridSpec(
                num_scalar_prefetch=1,
                grid=(2 * tiles,),
                in_specs=[
                    own_spec(head, False),
                    got_spec(head, True),
                    own_spec(head, False),
                    got_spec(head, True),
                    pl.BlockSpec((size, mine), lambda t, s: (t, 0)),
                    pieces_spec(),
                    pieces_spec(),
                ],
                out_specs=(pieces_spec(), pieces_spec()),
                scratch_shapes=[
                    pltpu.VMEM((width, 2 * width), BF16),
                    pltpu.VMEM((width, width), BF16),
                    pltpu.VMEM((width, 2 * width), F32),
                    pltpu.VMEM((width, width), F32),
                ],
            ),
            compiler_params=pltpu.CompilerParams(dimension_semantics=("arbitrary",)),
            cost_estimate=pl.CostEstimate(
                flops=28 * rows * width * width, transcendentals=4 * rows * width,
                bytes_accessed=8 * rows * width + 12 * width * width,
            ),
            name=f"learn{head}",
        )(where, keys, key_got, values, value_got, scale, own, got)

    def answer(head, own, got):
        side = jax.ShapeDtypeStruct((rows, width), BF16)
        return pl.pallas_call(
            functools.partial(answer_kernel, masks=masks[head], tiles=tiles),
            out_shape=(side, side),
            grid_spec=pltpu.PrefetchScalarGridSpec(
                num_scalar_prefetch=1,
                grid=(2 * tiles,),
                in_specs=[own_spec(head, True), got_spec(head, False), pieces_spec(), pieces_spec()],
                out_specs=(
                    pl.BlockSpec((size, width), lambda t, s: (jnp.maximum(t - tiles, 0), 0)),
                    pl.BlockSpec((size, width), lambda t, s: (jnp.minimum(t, tiles - 1), 0)),
                ),
                scratch_shapes=[
                    pltpu.VMEM((width, 2 * width), BF16),
                    pltpu.VMEM((width, width), BF16),
                    pltpu.VMEM((1, 2 * width), F32),
                    pltpu.VMEM((1, width), F32),
                ],
            ),
            compiler_params=pltpu.CompilerParams(dimension_semantics=("arbitrary",)),
            cost_estimate=pl.CostEstimate(
                flops=12 * rows * width * width, transcendentals=4 * rows * width,
                bytes_accessed=8 * rows * width + 6 * width * width,
            ),
            name=f"answer{head}",
        )(where, queries, query_got, own, got)

    outs_own = []
    outs_got = []
    for head in range(mine):
        keep, send = learn(head)
        summed = reduce_pieces(keep, send, masks[head], devices)
        fresh = (chip_rows[head].astype(F32) - summed).astype(BF16)
        own, got = gather_pieces(fresh, masks[head], devices)
        out_own, out_other = answer(head, own, got)
        outs_own.append(out_own)
        outs_got.append(flip(out_other, 1, devices))

    size_out = tile_of(rows, 256)
    return pl.pallas_call(
        functools.partial(norm_kernel, heads=mine),
        out_shape=jax.ShapeDtypeStruct((rows, heads * width), BF16),
        grid_spec=pltpu.PrefetchScalarGridSpec(
            num_scalar_prefetch=1,
            grid=(rows // size_out,),
            in_specs=[pl.BlockSpec((size_out, width), lambda t, s: (t, 0))] * (2 * mine)
            + [pl.BlockSpec((1, heads * width), lambda t, s: (0, 0))],
            out_specs=pl.BlockSpec((size_out, heads * width), lambda t, s: (t, 0)),
        ),
        compiler_params=pltpu.CompilerParams(dimension_semantics=("arbitrary",)),
        name="norm",
    )(where, *outs_own, *outs_got, out_gain[None, :])


def solution(mesh):
    in_specs = (
        P("tok", "head"),
        P("tok", "head"),
        P("tok", "head"),
        P("head", "tok"),
        P("head", "tok", None),
        P("head", "tok", None),
        P("head", "tok", None),
        P("head"),
    )
    out_specs = P("tok", "head")
    tok = mesh.shape["tok"]
    fast = mesh.shape["head"] == 1 and tok >= 8 and tok & (tok - 1) == 0
    body = fast_shards if fast else plain_shards
    return jax.shard_map(body, mesh=mesh, in_specs=in_specs, out_specs=out_specs, check_vma=False)
```

```python
import functools
import math

import jax
import jax.numpy as jnp
from jax import lax
from jax.experimental import pallas as pl
from jax.experimental.pallas import tpu as pltpu
from jax.sharding import PartitionSpec as P


F32 = jnp.float32
BF16 = jnp.bfloat16


def activate(gate):
    sigma = jax.nn.sigmoid(gate)
    return (gate * sigma, sigma * (1.0 + gate * (1.0 - sigma)))


def apply_heads(inputs, weights):
    return jnp.einsum("thi,hij->thj", inputs, weights, preferred_element_type=F32)


def scaled_columns(updated, norms):
    return (updated * lax.rsqrt(norms + 1e-06)[:, None, :]).astype(BF16)


def query_pass(query_rows, new_gate, new_up, new_down):
    query_gate = apply_heads(query_rows, new_gate)
    query_up = apply_heads(query_rows, new_up)
    query_act, _ = activate(query_gate)
    query_hidden = (query_act * query_up).astype(BF16)
    return apply_heads(query_hidden, new_down)


def plain_shards(queries, keys, values, rates, w_gate, w_up, w_down, out_gain):
    heads = w_gate.shape[0]
    width = w_gate.shape[2]
    rows = keys.shape[0]
    total = rows * lax.axis_size("tok")
    full_gate, full_up, full_down = (
        lax.all_gather(w_gate, "tok", axis=1, tiled=True),
        lax.all_gather(w_up, "tok", axis=1, tiled=True),
        lax.all_gather(w_down, "tok", axis=1, tiled=True),
    )
    key_rows = keys.reshape(rows, heads, width)
    value_rows = values.reshape(rows, heads, width).astype(F32)
    query_rows = queries.reshape(rows, heads, width)
    scale = rates.T / math.sqrt(total)
    gate = apply_heads(key_rows, full_gate)
    up = apply_heads(key_rows, full_up)
    act, slope = activate(gate)
    hidden = (act * up).astype(BF16)
    fitted = apply_heads(hidden, full_down)
    error = (scale[:, :, None] * (fitted - value_rows)).astype(BF16)
    grad_down = jnp.einsum("thi,thj->hij", hidden, error, preferred_element_type=F32)
    back = jnp.einsum("thj,hij->thi", error, full_down, preferred_element_type=F32)
    grad_gate = jnp.einsum(
        "thi,thj->hij", key_rows, (back * up * slope).astype(BF16), preferred_element_type=F32
    )
    grad_up = jnp.einsum("thi,thj->hij", key_rows, (back * act).astype(BF16), preferred_element_type=F32)
    sum_gate, sum_up, sum_down = lax.psum((grad_gate, grad_up, grad_down), "tok")
    updated = [
        full_gate.astype(F32) - sum_gate,
        full_up.astype(F32) - sum_up,
        full_down.astype(F32) - sum_down,
    ]
    new_gate, new_up, new_down = [scaled_columns(item, jnp.sum(item * item, axis=1)) for item in updated]
    applied = query_pass(query_rows, new_gate, new_up, new_down)
    flat = applied.reshape(rows, heads * width)
    square = lax.psum(jnp.sum(flat * flat, axis=1), "head")
    inverse = lax.rsqrt(square / (heads * width * lax.axis_size("head")) + 1e-06)
    return (flat * inverse[:, None] * out_gain[None, :]).astype(BF16)


def masks_of(chips, odd):
    planes = chips // 4
    masks = [4 << bit for bit in reversed(range(planes.bit_length() - 1))]
    return masks + ([1, 2] if odd else [2, 1])


def mask_of(piece, masks):
    value = 0
    for bit, mask in enumerate(masks):
        if piece >> bit & 1:
            value ^= mask
    return value


def flip(array, mask, devices):
    return lax.ppermute(array, "tok", [(i, i ^ mask) for i in range(devices)])


def gather_pieces(own, masks, devices):
    for stage, mask in enumerate(masks):
        got = flip(own, 2 * mask, devices)
        if stage == len(masks) - 1:
            return own, got
        own = jnp.concatenate([own, got], axis=0)


def gather_planes(own, masks, devices):
    own = own[:, None]
    for mask in masks:
        got = flip(own, 2 * mask, devices)
        own = jnp.concatenate([own, got], axis=1)
    return own


def add(a, b):
    return a.astype(F32) + b.astype(F32)


def reduce_pieces(keep, send, masks, devices):
    got = flip(send, 2 * masks[-1], devices)
    for mask in reversed(masks[1:-1]):
        half = keep.shape[0] // 2
        send = add(keep[half:], got[half:]).astype(BF16)
        keep = add(keep[:half], got[:half])
        got = flip(send, 2 * mask, devices)
    keep = add(keep, got)
    got = flip(keep.astype(BF16), 2 * masks[0], devices)
    return keep + jnp.stack([got[1], got[0]]).astype(F32)


def assemble(place_ref, own_ref, got_ref, wide_ref, down_ref, masks):
    pieces, _, rows, width = own_ref.shape
    chip = place_ref[1]
    for piece in range(2 * pieces):
        source = own_ref if piece < pieces else got_ref
        at = pl.multiple_of((chip ^ mask_of(piece, masks)) * rows, rows)
        index = piece % pieces
        wide_ref[pl.ds(at, rows), :width] = source[index, 0]
        wide_ref[pl.ds(at, rows), width:] = source[index, 1]
        down_ref[pl.ds(at, rows), :] = source[index, 2]


def contract_rows(a, b):
    return lax.dot_general(a, b, (((0,), (0,)), ((), ())), preferred_element_type=F32)


def learn_kernel(
    place_ref, k_own, k_got, v_own, v_got, scale_ref, own_ref, got_ref,
    keep_ref, send_ref, wide, down, grad_wide, grad_down, *, head, masks, out_masks, tiles,
):
    step = pl.program_id(0)
    width = down.shape[1]

    @pl.when(step == 0)
    def _():
        assemble(place_ref, own_ref, got_ref, wide, down, masks)
        grad_wide[...] = jnp.zeros_like(grad_wide)
        grad_down[...] = jnp.zeros_like(grad_down)

    def tile(k_ref, v_ref):
        k = k_ref[...]
        both = jnp.dot(k, wide[...], preferred_element_type=F32)
        gate = both[:, :width]
        up = both[:, width:]
        sigma = 1.0 / (1.0 + jnp.exp(-gate))
        act = gate * sigma
        hidden = (act * up).astype(BF16)
        fitted = jnp.dot(hidden, down[...], preferred_element_type=F32)
        scale = scale_ref[:, head : head + 1]
        error = (scale * (fitted - v_ref[...].astype(F32))).astype(BF16)
        grad_down[...] += contract_rows(hidden, error)
        back = lax.dot_general(
            error, down[...], (((1,), (1,)), ((), ())), preferred_element_type=F32
        )
        slope = sigma + act * (1.0 - sigma)
        dgate = (back * up * slope).astype(BF16)
        dup = (back * act).astype(BF16)
        grad_wide[:, :width] += contract_rows(k, dgate)
        grad_wide[:, width:] += contract_rows(k, dup)

    @pl.when(step < tiles)
    def _():
        tile(k_own, v_own)

    @pl.when(step >= tiles)
    def _():
        tile(k_got, v_got)

    @pl.when(step == 2 * tiles - 1)
    def _():
        pieces, _, rows, _ = keep_ref.shape
        chip = place_ref[1]
        for piece in range(2 * pieces):
            target = keep_ref if piece < pieces else send_ref
            at = pl.multiple_of((chip ^ mask_of(piece, out_masks)) * rows, rows)
            index = piece % pieces
            target[index, 0] = grad_wide[pl.ds(at, rows), :width].astype(target.dtype)
            target[index, 1] = grad_wide[pl.ds(at, rows), width:].astype(target.dtype)
            target[index, 2] = grad_down[pl.ds(at, rows), :].astype(target.dtype)


def answer_kernel(
    place_ref, q_own, q_got, own_ref, got_ref, out_own, out_other,
    wide, down, wide_norm, down_norm, *, masks, tiles,
):
    step = pl.program_id(0)
    width = down.shape[1]

    @pl.when(step == 0)
    def _():
        assemble(place_ref, own_ref, got_ref, wide, down, masks)
        first = wide[...].astype(F32)
        wide_norm[...] = lax.rsqrt(jnp.sum(first * first, axis=0, keepdims=True) + 1e-06)
        second = down[...].astype(F32)
        down_norm[...] = lax.rsqrt(jnp.sum(second * second, axis=0, keepdims=True) + 1e-06)

    def tile(q_ref, out_ref):
        both = jnp.dot(q_ref[...], wide[...], preferred_element_type=F32) * wide_norm[...]
        gate = both[:, :width]
        act = gate / (1.0 + jnp.exp(-gate))
        hidden = (act * both[:, width:]).astype(BF16)
        out = jnp.dot(hidden, down[...], preferred_element_type=F32) * down_norm[...]
        out_ref[...] = out.astype(BF16)

    @pl.when(step < tiles)
    def _():
        tile(q_got, out_other)

    @pl.when(step >= tiles)
    def _():
        tile(q_own, out_own)


def norm_kernel(place_ref, *refs, heads):
    own, got, gain_ref, out_ref = refs[:heads], refs[heads : 2 * heads], refs[-2], refs[-1]
    width = own[0].shape[1]
    total = 0.0
    for ref in own + got:
        block = ref[...].astype(F32)
        total = total + jnp.sum(block * block, axis=1, keepdims=True)
    inverse = lax.rsqrt(total / (2 * heads * width) + 1e-06)

    def write(first, second):
        for index, ref in enumerate(first + second):
            at = slice(index * width, (index + 1) * width)
            out_ref[:, at] = (ref[...].astype(F32) * inverse * gain_ref[:, at]).astype(BF16)

    @pl.when(place_ref[0] == 0)
    def _():
        write(own, got)

    @pl.when(place_ref[0] != 0)
    def _():
        write(got, own)


def tile_of(rows, most):
    size = most
    while rows % size:
        size //= 2
    return size


def fast_shards(*arrays):
    return fast_body(*arrays)


def fast_body(queries, keys, values, rates, w_gate, w_up, w_down, out_gain):
    heads, share, width = w_gate.shape
    if heads % 2:
        return plain_shards(queries, keys, values, rates, w_gate, w_up, w_down, out_gain)
    rows = keys.shape[0]
    devices = lax.axis_size("tok")
    chips = devices // 2
    mine = heads // 2
    total = rows * devices
    place = lax.axis_index("tok")
    core = place % 2
    chip = place // 2
    where = jnp.stack([core, chip]).astype(jnp.int32)

    def halves(array, axis, core):
        size = array.shape[axis] // 2
        keep = lax.dynamic_slice_in_dim(array, core * size, size, axis)
        give = lax.dynamic_slice_in_dim(array, (1 - core) * size, size, axis)
        return keep, flip(give, 1, devices)

    stacked = jnp.stack([w_gate, w_up, w_down], axis=1)
    kept, got = halves(stacked, 0, core)
    pair = jnp.where(core == 0, jnp.stack([kept, got], 2), jnp.stack([got, kept], 2))
    chip_rows = pair.reshape(mine, 3, 2 * share, width)

    masks = masks_of(chips, False)
    lead = len(masks) - 2
    late = masks_of(chips, True)
    early = late[:1] + [late[-2]] + late[1:-2] + late[-1:] if lead > 1 else late
    out_masks = [early if 2 * head < mine else late for head in range(mine)]
    planes = []
    groups = [1] * mine if mine < 4 or mine % 2 else [1, 1] + [2] * (mine // 2 - 1)
    head = 0
    for group in groups:
        both = gather_planes(chip_rows[head : head + group], masks[:lead], devices)
        planes += [both[index] for index in range(group)]
        head += group
    weights = [gather_pieces(planes[head], masks[lead:], devices) for head in range(mine)]

    own_rates, got_rates = halves(rates, 0, core)
    scale = jnp.concatenate([own_rates, got_rates], axis=1).T / math.sqrt(total)
    key_got = halves(keys, 1, core)[1]
    value_got = halves(values, 1, core)[1]

    size = tile_of(rows, 512)
    tiles = rows // size
    piece_rows = 2 * share
    half = chips // 2

    def pieces_spec():
        return pl.BlockSpec((half, 3, piece_rows, width), lambda t, s: (0, 0, 0, 0))

    def own_spec(head, late):
        if late:
            return pl.BlockSpec((size, width), lambda t, s: (jnp.maximum(t - tiles, 0), s[0] * mine + head))
        return pl.BlockSpec((size, width), lambda t, s: (jnp.minimum(t, tiles - 1), s[0] * mine + head))

    def got_spec(head, late):
        if late:
            return pl.BlockSpec((size, width), lambda t, s: (jnp.maximum(t - tiles, 0), head))
        return pl.BlockSpec((size, width), lambda t, s: (jnp.minimum(t, tiles - 1), head))

    def learn(head):
        own, got = weights[head]
        pieces = jax.ShapeDtypeStruct((half, 3, piece_rows, width), BF16)
        return pl.pallas_call(
            functools.partial(learn_kernel, head=head, masks=masks, out_masks=out_masks[head], tiles=tiles),
            out_shape=(jax.ShapeDtypeStruct(pieces.shape, F32), pieces),
            grid_spec=pltpu.PrefetchScalarGridSpec(
                num_scalar_prefetch=1,
                grid=(2 * tiles,),
                in_specs=[
                    own_spec(head, False),
                    got_spec(head, True),
                    own_spec(head, False),
                    got_spec(head, True),
                    pl.BlockSpec((size, mine), lambda t, s: (t, 0)),
                    pieces_spec(),
                    pieces_spec(),
                ],
                out_specs=(pieces_spec(), pieces_spec()),
                scratch_shapes=[
                    pltpu.VMEM((width, 2 * width), BF16),
                    pltpu.VMEM((width, width), BF16),
                    pltpu.VMEM((width, 2 * width), F32),
                    pltpu.VMEM((width, width), F32),
                ],
            ),
            compiler_params=pltpu.CompilerParams(dimension_semantics=("arbitrary",)),
            cost_estimate=pl.CostEstimate(
                flops=28 * rows * width * width, transcendentals=4 * rows * width,
                bytes_accessed=8 * rows * width + 12 * width * width,
            ),
        )(where, keys, key_got, values, value_got, scale, own, got)

    def answer(head, own, got):
        side = jax.ShapeDtypeStruct((rows, width), BF16)
        return pl.pallas_call(
            functools.partial(answer_kernel, masks=masks_of(chips, head % 2 == 0), tiles=tiles),
            out_shape=(side, side),
            grid_spec=pltpu.PrefetchScalarGridSpec(
                num_scalar_prefetch=1,
                grid=(2 * tiles,),
                in_specs=[own_spec(head, True), got_spec(head, False), pieces_spec(), pieces_spec()],
                out_specs=(
                    pl.BlockSpec((size, width), lambda t, s: (jnp.maximum(t - tiles, 0), 0)),
                    pl.BlockSpec((size, width), lambda t, s: (jnp.minimum(t, tiles - 1), 0)),
                ),
                scratch_shapes=[
                    pltpu.VMEM((width, 2 * width), BF16),
                    pltpu.VMEM((width, width), BF16),
                    pltpu.VMEM((1, 2 * width), F32),
                    pltpu.VMEM((1, width), F32),
                ],
            ),
            compiler_params=pltpu.CompilerParams(dimension_semantics=("arbitrary",)),
            cost_estimate=pl.CostEstimate(
                flops=12 * rows * width * width, transcendentals=4 * rows * width,
                bytes_accessed=8 * rows * width + 6 * width * width,
            ),
        )(where, queries, query_got, own, got)

    outs_own = []
    outs_got = []
    learned = []
    for head in range(mine):
        learned.append(learn(head))
    core_query = lax.optimization_barrier((core, learned[-1][1]))[0]
    query_got = halves(queries, 1, core_query)[1]
    for head in range(mine):
        keep, send = learned[head]
        summed = reduce_pieces(keep, send, out_masks[head], devices)
        fresh = (planes[head][: summed.shape[0]].astype(F32) - summed).astype(BF16)
        own, got = gather_pieces(fresh, masks_of(chips, head % 2 == 0)[1:], devices)
        out_own, out_other = answer(head, own, got)
        outs_own.append(out_own)
        outs_got.append(flip(out_other, 1, devices))

    size_out = tile_of(rows, 256)
    return pl.pallas_call(
        functools.partial(norm_kernel, heads=mine),
        out_shape=jax.ShapeDtypeStruct((rows, heads * width), BF16),
        grid_spec=pltpu.PrefetchScalarGridSpec(
            num_scalar_prefetch=1,
            grid=(rows // size_out,),
            in_specs=[pl.BlockSpec((size_out, width), lambda t, s: (t, 0))] * (2 * mine)
            + [pl.BlockSpec((1, heads * width), lambda t, s: (0, 0))],
            out_specs=pl.BlockSpec((size_out, heads * width), lambda t, s: (t, 0)),
        ),
        compiler_params=pltpu.CompilerParams(dimension_semantics=("arbitrary",)),
        name="norm",
    )(where, *outs_own, *outs_got, out_gain[None, :])


def solution(mesh):
    in_specs = (
        P("tok", "head"),
        P("tok", "head"),
        P("tok", "head"),
        P("head", "tok"),
        P("head", "tok", None),
        P("head", "tok", None),
        P("head", "tok", None),
        P("head"),
    )
    out_specs = P("tok", "head")
    tok = mesh.shape["tok"]
    fast = mesh.shape["head"] == 1 and tok >= 8 and tok & (tok - 1) == 0
    body = fast_shards if fast else plain_shards
    return jax.shard_map(body, mesh=mesh, in_specs=in_specs, out_specs=out_specs, check_vma=False)
```

```python
import functools
import math

import jax
import jax.numpy as jnp
from jax import lax
from jax.experimental import pallas as pl
from jax.experimental.pallas import tpu as pltpu
from jax.sharding import PartitionSpec as P


F32 = jnp.float32
BF16 = jnp.bfloat16


def activate(gate):
    sigma = jax.nn.sigmoid(gate)
    return (gate * sigma, sigma * (1.0 + gate * (1.0 - sigma)))


def apply_heads(inputs, weights):
    return jnp.einsum("thi,hij->thj", inputs, weights, preferred_element_type=F32)


def scaled_columns(updated, norms):
    return (updated * lax.rsqrt(norms + 1e-06)[:, None, :]).astype(BF16)


def query_pass(query_rows, new_gate, new_up, new_down):
    query_gate = apply_heads(query_rows, new_gate)
    query_up = apply_heads(query_rows, new_up)
    query_act, _ = activate(query_gate)
    query_hidden = (query_act * query_up).astype(BF16)
    return apply_heads(query_hidden, new_down)


def plain_shards(queries, keys, values, rates, w_gate, w_up, w_down, out_gain):
    heads = w_gate.shape[0]
    width = w_gate.shape[2]
    rows = keys.shape[0]
    total = rows * lax.axis_size("tok")
    full_gate, full_up, full_down = (
        lax.all_gather(w_gate, "tok", axis=1, tiled=True),
        lax.all_gather(w_up, "tok", axis=1, tiled=True),
        lax.all_gather(w_down, "tok", axis=1, tiled=True),
    )
    key_rows = keys.reshape(rows, heads, width)
    value_rows = values.reshape(rows, heads, width).astype(F32)
    query_rows = queries.reshape(rows, heads, width)
    scale = rates.T / math.sqrt(total)
    gate = apply_heads(key_rows, full_gate)
    up = apply_heads(key_rows, full_up)
    act, slope = activate(gate)
    hidden = (act * up).astype(BF16)
    fitted = apply_heads(hidden, full_down)
    error = (scale[:, :, None] * (fitted - value_rows)).astype(BF16)
    grad_down = jnp.einsum("thi,thj->hij", hidden, error, preferred_element_type=F32)
    back = jnp.einsum("thj,hij->thi", error, full_down, preferred_element_type=F32)
    grad_gate = jnp.einsum(
        "thi,thj->hij", key_rows, (back * up * slope).astype(BF16), preferred_element_type=F32
    )
    grad_up = jnp.einsum("thi,thj->hij", key_rows, (back * act).astype(BF16), preferred_element_type=F32)
    sum_gate, sum_up, sum_down = lax.psum((grad_gate, grad_up, grad_down), "tok")
    updated = [
        full_gate.astype(F32) - sum_gate,
        full_up.astype(F32) - sum_up,
        full_down.astype(F32) - sum_down,
    ]
    new_gate, new_up, new_down = [scaled_columns(item, jnp.sum(item * item, axis=1)) for item in updated]
    applied = query_pass(query_rows, new_gate, new_up, new_down)
    flat = applied.reshape(rows, heads * width)
    square = lax.psum(jnp.sum(flat * flat, axis=1), "head")
    inverse = lax.rsqrt(square / (heads * width * lax.axis_size("head")) + 1e-06)
    return (flat * inverse[:, None] * out_gain[None, :]).astype(BF16)


def masks_of(chips, odd):
    planes = chips // 4
    masks = [4 << bit for bit in reversed(range(planes.bit_length() - 1))]
    return masks + ([1, 2] if odd else [2, 1])


def mask_of(piece, masks):
    value = 0
    for bit, mask in enumerate(masks):
        if piece >> bit & 1:
            value ^= mask
    return value


def flip(array, mask, devices):
    return lax.ppermute(array, "tok", [(i, i ^ mask) for i in range(devices)])


def gather_pieces(own, masks, devices):
    for stage, mask in enumerate(masks):
        got = flip(own, 2 * mask, devices)
        if stage == len(masks) - 1:
            return own, got
        own = jnp.concatenate([own, got], axis=0)


def gather_planes(own, masks, devices):
    own = own[:, None]
    for mask in masks:
        got = flip(own, 2 * mask, devices)
        own = jnp.concatenate([own, got], axis=1)
    return own


def add(a, b):
    return a.astype(F32) + b.astype(F32)


def reduce_pieces(keep, send, masks, devices):
    got = flip(send, 2 * masks[-1], devices)
    for mask in reversed(masks[1:-1]):
        half = keep.shape[0] // 2
        send = add(keep[half:], got[half:]).astype(BF16)
        keep = add(keep[:half], got[:half])
        got = flip(send, 2 * mask, devices)
    keep = add(keep, got)
    got = flip(keep.astype(BF16), 2 * masks[0], devices)
    return keep + jnp.stack([got[1], got[0]]).astype(F32)


def assemble(place_ref, own_ref, got_ref, wide_ref, down_ref, masks):
    pieces, _, rows, width = own_ref.shape
    chip = place_ref[1]
    for piece in range(2 * pieces):
        source = own_ref if piece < pieces else got_ref
        at = pl.multiple_of((chip ^ mask_of(piece, masks)) * rows, rows)
        index = piece % pieces
        wide_ref[pl.ds(at, rows), :width] = source[index, 0]
        wide_ref[pl.ds(at, rows), width:] = source[index, 1]
        down_ref[pl.ds(at, rows), :] = source[index, 2]


def contract_rows(a, b):
    return lax.dot_general(a, b, (((0,), (0,)), ((), ())), preferred_element_type=F32)


def learn_kernel(
    place_ref, k_own, k_got, v_own, v_got, scale_ref, own_ref, got_ref,
    keep_ref, send_ref, wide, down, grad_wide, grad_down, *, head, masks, out_masks, tiles,
):
    step = pl.program_id(0)
    width = down.shape[1]

    @pl.when(step == 0)
    def _():
        assemble(place_ref, own_ref, got_ref, wide, down, masks)
        grad_wide[...] = jnp.zeros_like(grad_wide)
        grad_down[...] = jnp.zeros_like(grad_down)

    def tile(k, v):
        both = jnp.dot(k, wide[...], preferred_element_type=F32)
        gate = both[:, :width]
        up = both[:, width:]
        sigma = 1.0 / (1.0 + jnp.exp(-gate))
        act = gate * sigma
        hidden = (act * up).astype(BF16)
        fitted = jnp.dot(hidden, down[...], preferred_element_type=F32)
        scale = scale_ref[:, head : head + 1]
        error = (scale * (fitted - v.astype(F32))).astype(BF16)
        grad_down[...] += contract_rows(hidden, error)
        back = lax.dot_general(
            error, down[...], (((1,), (1,)), ((), ())), preferred_element_type=F32
        )
        slope = sigma + act * (1.0 - sigma)
        dgate = (back * up * slope).astype(BF16)
        dup = (back * act).astype(BF16)
        grad_wide[:, :width] += contract_rows(k, dgate)
        grad_wide[:, width:] += contract_rows(k, dup)

    early = step < tiles
    tile(jnp.where(early, k_own[...], k_got[...]), jnp.where(early, v_own[...], v_got[...]))

    @pl.when(step == 2 * tiles - 1)
    def _():
        pieces, _, rows, _ = keep_ref.shape
        chip = place_ref[1]
        for piece in range(2 * pieces):
            target = keep_ref if piece < pieces else send_ref
            at = pl.multiple_of((chip ^ mask_of(piece, out_masks)) * rows, rows)
            index = piece % pieces
            target[index, 0] = grad_wide[pl.ds(at, rows), :width].astype(target.dtype)
            target[index, 1] = grad_wide[pl.ds(at, rows), width:].astype(target.dtype)
            target[index, 2] = grad_down[pl.ds(at, rows), :].astype(target.dtype)


def answer_kernel(
    place_ref, q_own, q_got, own_ref, got_ref, out_own, out_other,
    wide, down, wide_norm, down_norm, *, masks, tiles,
):
    step = pl.program_id(0)
    width = down.shape[1]

    @pl.when(step == 0)
    def _():
        assemble(place_ref, own_ref, got_ref, wide, down, masks)
        first = wide[...].astype(F32)
        wide_norm[...] = lax.rsqrt(jnp.sum(first * first, axis=0, keepdims=True) + 1e-06)
        second = down[...].astype(F32)
        down_norm[...] = lax.rsqrt(jnp.sum(second * second, axis=0, keepdims=True) + 1e-06)

    q = jnp.where(step < tiles, q_got[...], q_own[...])
    both = jnp.dot(q, wide[...], preferred_element_type=F32) * wide_norm[...]
    gate = both[:, :width]
    act = gate / (1.0 + jnp.exp(-gate))
    hidden = (act * both[:, width:]).astype(BF16)
    out = (jnp.dot(hidden, down[...], preferred_element_type=F32) * down_norm[...]).astype(BF16)

    @pl.when(step < tiles)
    def _():
        out_other[...] = out

    @pl.when(step >= tiles)
    def _():
        out_own[...] = out


def norm_kernel(place_ref, *refs, heads):
    own, got, gain_ref, out_ref = refs[:heads], refs[heads : 2 * heads], refs[-2], refs[-1]
    width = own[0].shape[1]
    total = 0.0
    for ref in own + got:
        block = ref[...].astype(F32)
        total = total + jnp.sum(block * block, axis=1, keepdims=True)
    inverse = lax.rsqrt(total / (2 * heads * width) + 1e-06)

    def write(first, second):
        for index, ref in enumerate(first + second):
            at = slice(index * width, (index + 1) * width)
            out_ref[:, at] = (ref[...].astype(F32) * inverse * gain_ref[:, at]).astype(BF16)

    @pl.when(place_ref[0] == 0)
    def _():
        write(own, got)

    @pl.when(place_ref[0] != 0)
    def _():
        write(got, own)


def tile_of(rows, most):
    size = most
    while rows % size:
        size //= 2
    return size


def fast_shards(*arrays):
    return fast_body(*arrays)


def fast_body(queries, keys, values, rates, w_gate, w_up, w_down, out_gain):
    heads, share, width = w_gate.shape
    if heads % 2:
        return plain_shards(queries, keys, values, rates, w_gate, w_up, w_down, out_gain)
    rows = keys.shape[0]
    devices = lax.axis_size("tok")
    chips = devices // 2
    mine = heads // 2
    total = rows * devices
    place = lax.axis_index("tok")
    core = place % 2
    chip = place // 2
    where = jnp.stack([core, chip]).astype(jnp.int32)

    def halves(array, axis, core):
        size = array.shape[axis] // 2
        keep = lax.dynamic_slice_in_dim(array, core * size, size, axis)
        give = lax.dynamic_slice_in_dim(array, (1 - core) * size, size, axis)
        return keep, flip(give, 1, devices)

    stacked = jnp.stack([w_gate, w_up, w_down], axis=1)
    kept, got = halves(stacked, 0, core)
    pair = jnp.where(core == 0, jnp.stack([kept, got], 2), jnp.stack([got, kept], 2))
    chip_rows = pair.reshape(mine, 3, 2 * share, width)

    masks = masks_of(chips, False)
    lead = len(masks) - 2
    late = masks_of(chips, True)
    early = late[:1] + [late[-2]] + late[1:-2] + late[-1:] if lead > 1 else late
    out_masks = [early if 2 * head < mine else late for head in range(mine)]
    planes = []
    groups = [1] * mine if mine < 4 or mine % 2 else [1, 1] + [2] * (mine // 2 - 1)
    head = 0
    for group in groups:
        both = gather_planes(chip_rows[head : head + group], masks[:lead], devices)
        planes += [both[index] for index in range(group)]
        head += group
    weights = [gather_pieces(planes[head], masks[lead:], devices) for head in range(mine)]

    own_rates, got_rates = halves(rates, 0, core)
    scale = jnp.concatenate([own_rates, got_rates], axis=1).T / math.sqrt(total)
    key_got = halves(keys, 1, core)[1]
    value_got = halves(values, 1, core)[1]

    size = tile_of(rows, 512)
    tiles = rows // size
    piece_rows = 2 * share
    half = chips // 2

    def pieces_spec():
        return pl.BlockSpec((half, 3, piece_rows, width), lambda t, s: (0, 0, 0, 0))

    def own_spec(head, late):
        if late:
            return pl.BlockSpec((size, width), lambda t, s: (jnp.maximum(t - tiles, 0), s[0] * mine + head))
        return pl.BlockSpec((size, width), lambda t, s: (jnp.minimum(t, tiles - 1), s[0] * mine + head))

    def got_spec(head, late):
        if late:
            return pl.BlockSpec((size, width), lambda t, s: (jnp.maximum(t - tiles, 0), head))
        return pl.BlockSpec((size, width), lambda t, s: (jnp.minimum(t, tiles - 1), head))

    def learn(head):
        own, got = weights[head]
        pieces = jax.ShapeDtypeStruct((half, 3, piece_rows, width), BF16)
        return pl.pallas_call(
            functools.partial(learn_kernel, head=head, masks=masks, out_masks=out_masks[head], tiles=tiles),
            out_shape=(jax.ShapeDtypeStruct(pieces.shape, F32), pieces),
            grid_spec=pltpu.PrefetchScalarGridSpec(
                num_scalar_prefetch=1,
                grid=(2 * tiles,),
                in_specs=[
                    own_spec(head, False),
                    got_spec(head, True),
                    own_spec(head, False),
                    got_spec(head, True),
                    pl.BlockSpec((size, mine), lambda t, s: (t, 0)),
                    pieces_spec(),
                    pieces_spec(),
                ],
                out_specs=(pieces_spec(), pieces_spec()),
                scratch_shapes=[
                    pltpu.VMEM((width, 2 * width), BF16),
                    pltpu.VMEM((width, width), BF16),
                    pltpu.VMEM((width, 2 * width), F32),
                    pltpu.VMEM((width, width), F32),
                ],
            ),
            compiler_params=pltpu.CompilerParams(dimension_semantics=("arbitrary",)),
            cost_estimate=pl.CostEstimate(
                flops=28 * rows * width * width, transcendentals=4 * rows * width,
                bytes_accessed=8 * rows * width + 12 * width * width,
            ),
        )(where, keys, key_got, values, value_got, scale, own, got)

    def answer(head, own, got):
        side = jax.ShapeDtypeStruct((rows, width), BF16)
        return pl.pallas_call(
            functools.partial(answer_kernel, masks=masks_of(chips, (head % 2 == 0) != (2 * head >= mine)), tiles=tiles),
            out_shape=(side, side),
            grid_spec=pltpu.PrefetchScalarGridSpec(
                num_scalar_prefetch=1,
                grid=(2 * tiles,),
                in_specs=[own_spec(head, True), got_spec(head, False), pieces_spec(), pieces_spec()],
                out_specs=(
                    pl.BlockSpec((size, width), lambda t, s: (jnp.maximum(t - tiles, 0), 0)),
                    pl.BlockSpec((size, width), lambda t, s: (jnp.minimum(t, tiles - 1), 0)),
                ),
                scratch_shapes=[
                    pltpu.VMEM((width, 2 * width), BF16),
                    pltpu.VMEM((width, width), BF16),
                    pltpu.VMEM((1, 2 * width), F32),
                    pltpu.VMEM((1, width), F32),
                ],
            ),
            compiler_params=pltpu.CompilerParams(dimension_semantics=("arbitrary",)),
            cost_estimate=pl.CostEstimate(
                flops=12 * rows * width * width, transcendentals=4 * rows * width,
                bytes_accessed=8 * rows * width + 6 * width * width,
            ),
        )(where, queries, query_got, own, got)

    outs_own = []
    outs_got = []
    learned = []
    for head in range(mine):
        learned.append(learn(head))
    core_query = lax.optimization_barrier((core, learned[-1][1]))[0]
    query_got = halves(queries, 1, core_query)[1]
    for head in range(mine):
        keep, send = learned[head]
        summed = reduce_pieces(keep, send, out_masks[head], devices)
        fresh = (planes[head][: summed.shape[0]].astype(F32) - summed).astype(BF16)
        own, got = gather_pieces(fresh, masks_of(chips, (head % 2 == 0) != (2 * head >= mine))[1:], devices)
        out_own, out_other = answer(head, own, got)
        outs_own.append(out_own)
        outs_got.append(flip(out_other, 1, devices))

    size_out = tile_of(rows, 256)
    return pl.pallas_call(
        functools.partial(norm_kernel, heads=mine),
        out_shape=jax.ShapeDtypeStruct((rows, heads * width), BF16),
        grid_spec=pltpu.PrefetchScalarGridSpec(
            num_scalar_prefetch=1,
            grid=(rows // size_out,),
            in_specs=[pl.BlockSpec((size_out, width), lambda t, s: (t, 0))] * (2 * mine)
            + [pl.BlockSpec((1, heads * width), lambda t, s: (0, 0))],
            out_specs=pl.BlockSpec((size_out, heads * width), lambda t, s: (t, 0)),
        ),
        compiler_params=pltpu.CompilerParams(dimension_semantics=("arbitrary",)),
        name="norm",
    )(where, *outs_own, *outs_got, out_gain[None, :])


def solution(mesh):
    in_specs = (
        P("tok", "head"),
        P("tok", "head"),
        P("tok", "head"),
        P("head", "tok"),
        P("head", "tok", None),
        P("head", "tok", None),
        P("head", "tok", None),
        P("head"),
    )
    out_specs = P("tok", "head")
    tok = mesh.shape["tok"]
    fast = mesh.shape["head"] == 1 and tok >= 8 and tok & (tok - 1) == 0
    body = fast_shards if fast else plain_shards
    return jax.shard_map(body, mesh=mesh, in_specs=in_specs, out_specs=out_specs, check_vma=False)
```
